128 devices in a mesh: dom: 32 (over z, y, core), col: 2 (over x_hi), batch: 2 (over x_lo).
Axes of the slice: x: 4 (x_hi: 2, x_lo: 2; x = x_hi * 2 + x_lo), y: 4, z: 4, core: 2. Of those that a mesh axis runs over, the one named last changes fastest.
Arguments:
- features: bfloat16 [65536, 128], P('dom', 'col'), may hold values from -6 to 6
- self_weight1: bfloat16 [128, 256], P('col', 'batch'), may hold values from -0.5 to 0.5
- neigh_weight1: bfloat16 [128, 256], P('col', 'batch'), may hold values from -2 to 2
- need_first: int32 [64, 64], P(('dom', 'batch')), may hold values from 0 to 511, as said below
- count_first: int32 [64], P(('dom', 'batch')), may hold values from 0 to 64
- adjacency_first: int32 [65536, 512], P(('dom', 'batch')), may hold values from 0 to 16384, as said below
- self_weight2: bfloat16 [256, 172], P('col', 'batch'), may hold values from -0.375 to 0.375
- neigh_weight2: bfloat16 [256, 172], P('col', 'batch'), may hold values from -0.375 to 0.375
- need_second: int32 [64, 64], P(('dom', 'batch')), may hold values from 0 to 511, as said below
- count_second: int32 [64], P(('dom', 'batch')), may hold values from 0 to 64
- adjacency_second: int32 [65536, 512], P(('dom', 'batch')), may hold values from 0 to 16384, as said below
- seed_rows: int32 [65536], P(('dom', 'batch')), may hold values from 0 to 2047
Outputs:
- logits: float32 [65536, 172], P(('dom', 'batch'))
The draws below stay inside these ranges and needn't reach their ends.
Inputs may be any that keep to these rules, and one draw needn't show every extreme that they name: `need_first`: each row lists 64 different node blocks in increasing order; block g holds nodes 128 * g to 128 * g + 127 and lies in partition g // 16. At most 4 entries of one row lie in one partition, and exactly 4 lie in some partition in every row. `need_second`: each row lists 64 different frontier blocks in increasing order; block g holds frontier rows 128 * g to 128 * g + 127 and lies in partition g // 16. At most 4 entries of one row lie in one partition, and exactly 4 lie in some partition in every row. `adjacency_first`: bit i of word k of a row is the adjacency entry of column 16 k + i; at most one bit of a word is set, and bit 15 never. `adjacency_second`: bit i of word k of a row is the adjacency entry of column 16 k + i; at most one bit of a word is set, and bit 15 never.
All inputs are finite; a program needn't handle non-finite values.
Results may differ from the reference program's by a relative error of at most 0.0036.
Values may be sent and summed in bfloat16 or wider, within the bound.
A program may use at most 128 MiB of HBM per device.

```python
import math
import jax
import jax.numpy as jnp
from jax import lax

F = 128
HID = 256
CLASSES = 172
BLK = 128
NB_DEV = 16
T1_DEV = 1024
SEED_DEV = 1024
NEED1 = 64
NEED2 = 64
NODE_DEV = 2048
NODES = 65536
SEEDS = 65536
N_DOM = 32
N_BATCH = 2


def block_lists(key, rows, need_len, owners, owned):
    capacity = max(2, (2 * need_len + owners - 1) // owners)

    def one_row(row_key):
        key_list = jax.random.split(row_key, 4)
        boost_by = jax.random.randint(key_list[0], (owners,), 0, 4) * 2 ** 20
        leader = jax.random.randint(key_list[1], (), 0, owners)
        boost_by = jnp.where(jnp.arange(owners) == leader, 8 * 2 ** 20, boost_by)
        candidate_owner = jnp.arange(owners * capacity) // capacity
        scores = boost_by[candidate_owner] + jax.random.randint(key_list[2], (owners * capacity,), 0, 2 ** 20)
        ranking = jnp.argsort(-scores, stable=True)
        picked = ranking[:need_len]
        picked_owner = picked // capacity
        picked_rank = picked % capacity
        shuffle_scores = jax.random.randint(key_list[3], (owners, owned), 0, 2 ** 20)
        shuffles = jnp.argsort(shuffle_scores, axis=1, stable=True)
        local_block = shuffles[picked_owner, picked_rank]
        return jnp.sort(picked_owner * owned + local_block).astype(jnp.int32)
    return jax.vmap(one_row)(jax.random.split(key, rows))


def packed_adjacency(key, rows, width, columns):
    spread = max(16, columns // 24)
    drawn = jax.random.randint(key, (rows, width), 0, spread)
    single = jnp.left_shift(jnp.ones_like(drawn), jnp.minimum(drawn, 14))
    return jnp.where(drawn < 15, single, 0).astype(jnp.int32)


def draw_need_first(key, part):
    return block_lists(jax.random.fold_in(key, 11), N_DOM * N_BATCH, NEED1, N_DOM, NB_DEV)


def draw_need_second(key, part):
    return block_lists(jax.random.fold_in(key, 23), N_DOM * N_BATCH, NEED2, N_DOM, N_BATCH * T1_DEV // BLK)


def draw_adjacency_first(key, part):
    return packed_adjacency(jax.random.fold_in(key, 37), N_DOM * N_BATCH * T1_DEV, NEED1 * BLK // 16, NEED1 * BLK)


def draw_adjacency_second(key, part):
    return packed_adjacency(jax.random.fold_in(key, 41), N_DOM * N_BATCH * SEED_DEV, NEED2 * BLK // 16, NEED2 * BLK)


def touch_ends(values, rng, least, largest):
    longest = values.shape.index(max(values.shape))
    spots = []
    for shift in (0, 1):
        where = [jax.random.randint(jax.random.fold_in(rng, axis), (), 0, length) for axis, length in enumerate(values.shape)]
        where[longest] = (where[longest] + shift) % values.shape[longest]
        spots.append(tuple(where))
    return values.at[spots[0]].set(least).at[spots[1]].set(largest)


def block_scale(stream_key, shape, pieces, least, high):
    def one(axis_at, shards_of):
        heights = jax.random.uniform(jax.random.fold_in(jax.random.fold_in(stream_key, 6), axis_at), (shards_of,), jnp.float32, least / len(pieces), high / len(pieces))
        return jnp.repeat(jnp.exp(heights), shape[axis_at] // shards_of).reshape((-1,) + (1,) * (len(shape) - axis_at - 1))

    factor_of = one(*pieces[0])
    for cut in pieces[1:]:
        factor_of = factor_of * one(*cut)
    return factor_of


def gaussian(key, dims, scale, bound, pieces=(), held_as=jnp.bfloat16):
    values = scale * jax.random.normal(key, dims, jnp.float32)
    if pieces:
        values = values * block_scale(key, dims, pieces, -0.22, 0.18)
    return jnp.clip(values, -bound, bound).astype(held_as)


def setup_inputs(seed: int = 0) -> dict:
    arg_keys = jax.random.split(jax.random.key(seed), 13)
    features = gaussian(arg_keys[0], (NODES, F), 1.0, 6.0, ((0, 32), (1, 2)))
    self_weight1 = gaussian(arg_keys[1], (F, HID), F ** -0.5, 0.5, ((0, 2), (1, 2)))
    neigh_weight1 = gaussian(arg_keys[2], (F, HID), (F // 16) ** -0.5, 2.0, ((0, 2), (1, 2)))
    need_first = draw_need_first(jax.random.fold_in(arg_keys[12], 71), 0)
    count_first = touch_ends(jax.random.randint(arg_keys[4], (N_DOM * N_BATCH,), 0, NEED1 + 1), jax.random.fold_in(arg_keys[4], 1), 0, NEED1).astype(jnp.int32)
    adjacency_first = draw_adjacency_first(jax.random.fold_in(arg_keys[12], 71), 0)
    self_weight2 = gaussian(arg_keys[6], (HID, CLASSES), HID ** -0.5, 0.375, ((0, 2), (1, 2)))
    neigh_weight2 = gaussian(arg_keys[7], (HID, CLASSES), HID ** -0.5, 0.375, ((0, 2), (1, 2)))
    need_second = draw_need_second(jax.random.fold_in(arg_keys[12], 71), 0)
    count_second = touch_ends(jax.random.randint(arg_keys[9], (N_DOM * N_BATCH,), 0, NEED2 + 1), jax.random.fold_in(arg_keys[9], 1), 0, NEED2).astype(jnp.int32)
    adjacency_second = draw_adjacency_second(jax.random.fold_in(arg_keys[12], 71), 0)
    seed_rows = touch_ends(jax.random.randint(arg_keys[11], (SEEDS,), 0, N_BATCH * T1_DEV), jax.random.fold_in(arg_keys[11], 1), 0, (N_BATCH * T1_DEV) - 1).astype(jnp.int32)
    return {"features": features, "self_weight1": self_weight1, "neigh_weight1": neigh_weight1, "need_first": need_first, "count_first": count_first, "adjacency_first": adjacency_first, "self_weight2": self_weight2, "neigh_weight2": neigh_weight2, "need_second": need_second, "count_second": count_second, "adjacency_second": adjacency_second, "seed_rows": seed_rows}


def unpack_rows(packed_rows, valid_cols):
    shifts = jnp.arange(16, dtype=jnp.int32)
    bit_table = jnp.right_shift(packed_rows[:, :, None], shifts[None, None, :]) & 1
    bit_table = bit_table.reshape(packed_rows.shape[0], packed_rows.shape[1] * 16)
    column = jnp.arange(bit_table.shape[1], dtype=jnp.int32)
    return jnp.where(column[None, :] < valid_cols, bit_table, 0)


def mean_rows(packed, valid_cols, needed):
    total_rows = packed.shape[0]
    row_block = math.gcd(total_rows, 256)
    grouped = packed.reshape(total_rows // row_block, row_block, packed.shape[1])

    def one_block(row_piece):
        dense_rows = unpack_rows(row_piece, valid_cols)
        degree = jnp.sum(dense_rows, axis=1).astype(jnp.float32)
        summed = jnp.dot(dense_rows.astype(jnp.bfloat16), needed, preferred_element_type=jnp.float32)
        return (summed / jnp.maximum(degree, 1.0)[:, None]).astype(jnp.bfloat16)

    return lax.map(one_block, grouped).reshape(total_rows, needed.shape[1])


def layer_means(packed_all, counts, lists, blocks, rows_dev):
    workers = counts.shape[0]
    width = blocks.shape[1] // BLK

    def per_worker(worker):
        packed = lax.dynamic_slice_in_dim(packed_all, worker * rows_dev, rows_dev, 0)
        chosen = jnp.take(blocks, lists[worker], axis=0)
        needed = chosen.reshape(chosen.shape[0] * BLK, width)
        return mean_rows(packed, counts[worker] * BLK, needed)

    return lax.map(per_worker, jnp.arange(workers, dtype=jnp.int32)).reshape(workers * rows_dev, width)


def reference(features, self_weight1, neigh_weight1, need_first, count_first, adjacency_first, self_weight2, neigh_weight2, need_second, count_second, adjacency_second, seed_rows):
    workers = N_DOM * N_BATCH
    node_blocks = features.reshape(N_DOM * NB_DEV, BLK * F)
    near_first = layer_means(adjacency_first, count_first, need_first, node_blocks, T1_DEV)
    worker_ids = jnp.arange(workers, dtype=jnp.int32)
    starts = (worker_ids // N_BATCH) * NODE_DEV + (worker_ids % N_BATCH) * T1_DEV
    self_first = lax.map(lambda row_start: lax.dynamic_slice_in_dim(features, row_start, T1_DEV, 0), starts)
    self_first = self_first.reshape(workers * T1_DEV, F)
    pre_first = jnp.dot(self_first, self_weight1, preferred_element_type=jnp.float32) + jnp.dot(near_first, neigh_weight1, preferred_element_type=jnp.float32)
    hidden_first = jnp.maximum(pre_first, 0.0).astype(jnp.bfloat16)
    front_blocks = hidden_first.reshape(workers * T1_DEV // BLK, BLK * HID)
    near_second = layer_means(adjacency_second, count_second, need_second, front_blocks, SEED_DEV)
    seed_owner = jnp.arange(workers * SEED_DEV, dtype=jnp.int32) // SEED_DEV
    own_rows = (seed_owner // N_BATCH) * (N_BATCH * T1_DEV) + seed_rows
    own_second = jnp.take(hidden_first, own_rows, axis=0)
    logits = jnp.dot(own_second, self_weight2, preferred_element_type=jnp.float32) + jnp.dot(near_second, neigh_weight2, preferred_element_type=jnp.float32)
    return logits
```

```python
import jax
import jax.numpy as jnp
from jax import lax
from jax.experimental import pallas as pl
from jax.experimental.pallas import tpu as pltpu
from jax.sharding import PartitionSpec as P

MESH = pl.DeviceIdType.MESH
BF = jnp.bfloat16
F32 = jnp.float32
I32 = jnp.int32
ROWS = 1024
RB = 256
WORDS = 512
CQ = 43


def lane_groups(count, width, lanes):
    lane = lax.broadcasted_iota(I32, (1, lanes), 1)
    return [
        jnp.where((lane >= j * width) & (lane < (j + 1) * width), 1.0, 0.0).astype(BF)
        for j in range(count)
    ]


def quarter_of(index):
    return sum((index >= CQ * m).astype(I32) for m in range(1, 5))


def ones_at(hit):
    return jnp.where(hit, 1.0, 0.0).astype(BF)


def dot(a, b):
    return jnp.dot(a, b, preferred_element_type=F32)


def kernel(
    need_s, need_v, xs, a1, a2, aq, w, out,
    gx0, gx1, gx2, gx3, gp0, gp1, gp2, a1o, a2o, aqo, wg, need_r, need_o, sx, npk, ng, acc1, nr, acc2, accq,
    lhs, rhs1, rhs2, rhsq, sel1, sel2, wr, hid, pm, rg, lm, lgot,
    rx, ssx, sib1, rp, ssp, sib2, mr, ms, lsem,
):
    gx, gp = (gx0, gx1, gx2, gx3), (gp0, gp1, gp2)
    dom = lax.axis_index("dom")
    b = lax.axis_index("batch")
    c = lax.axis_index("col")
    core = dom % 2
    s1, s2 = 2 + 6 * core, 8 - 6 * core
    p1, p2 = (dom // s1) % 4, (dom // s2) % 4

    def at(d1, d2):
        return dom + s1 * ((p1 + d1) % 4 - p1) + s2 * ((p2 + d2) % 4 - p2)

    sib = dom + 1 - 2 * core
    rel = [
        (1 - b, c, {"col": c, "batch": 1 - b}),
        (b, 1 - c, {"col": 1 - c, "batch": b}),
        (1 - b, 1 - c, {"col": 1 - c, "batch": 1 - b}),
    ]
    q = 2 * c + b
    ts = 2 * b + c

    barrier = pltpu.get_barrier_semaphore()
    for n in (at(1, 0), at(3, 0), at(0, 1), at(0, 3), sib):
        pl.semaphore_signal(barrier, inc=1, device_id={"dom": n}, device_id_type=MESH)
    for _, _, dev in rel:
        pl.semaphore_signal(barrier, inc=1, device_id=dev, device_id_type=MESH)
    pl.semaphore_wait(barrier, 8)

    started = []

    def xchg(k, e, src, dst):
        cp = pltpu.make_async_remote_copy(
            src_ref=src, dst_ref=dst, send_sem=ms.at[k], recv_sem=mr.at[k],
            device_id=rel[e][2], device_id_type=MESH,
        )
        cp.start()
        started.append(cp)
        return cp

    def gather_over_dom(g, chunks, rsem, ssem, bsem, own):
        def copy(t, src, target, rs, first=False):
            pltpu.make_async_remote_copy(
                src_ref=own(t) if first else part(t, src), dst_ref=part(t, src),
                send_sem=ssem.at[t], recv_sem=rs, device_id={"dom": target}, device_id_type=MESH,
            ).start()

        def part(t, src, count=1):
            return g[t].at[pl.ds(pl.multiple_of(8 * src, 8), 8 * count)]

        def slot(t, d1, d2):
            return rsem.at[t, 4 * d1 + d2]

        def arrived(t, d1, d2):
            pltpu.make_async_copy(part(t, 0), part(t, 0), slot(t, d1, d2)).wait()

        def to_sib(t, d1, d2):
            copy(t, at(d1, d2), sib, bsem.at[t])

        def spread(t, d1):
            copy(t, at(d1, 0), at(0, 1), slot(t, d1, 3))
            copy(t, at(d1, 0), at(0, 3), slot(t, d1, 1))

        def pass_on(t, d1):
            f = 3 - 2 * ((t + d1) % 2)
            copy(t, at(d1, f), at(0, 4 - f), slot(t, d1, 2))

        def stage_a(t):
            copy(t, dom, at(1, 0), slot(t, 3, 0), True)
            copy(t, dom, at(3, 0), slot(t, 1, 0), True)
            copy(t, dom, at(0, 1), slot(t, 0, 3), True)
            copy(t, dom, at(0, 3), slot(t, 0, 1), True)
            copy(t, dom, sib, bsem.at[t], True)

        def stage_b(t):
            for d1 in (1, 3):
                arrived(t, d1, 0)
                spread(t, d1)
            f = 3 - 2 * (t % 2)
            copy(t, at(f, 0), at(4 - f, 0), slot(t, 2, 0))
            for d2 in (1, 3):
                arrived(t, 0, d2)
            pass_on(t, 0)
            for d in (1, 3):
                to_sib(t, d, 0)
                to_sib(t, 0, d)

        def stage_c(t):
            arrived(t, 2, 0)
            spread(t, 2)
            for d1 in (1, 3):
                arrived(t, d1, 1)
                arrived(t, d1, 3)
                pass_on(t, d1)
            arrived(t, 0, 2)
            to_sib(t, 2, 0)
            to_sib(t, 0, 2)
            for d1 in (1, 3):
                to_sib(t, d1, 1)
                to_sib(t, d1, 3)

        def stage_d(t):
            arrived(t, 2, 1)
            arrived(t, 2, 3)
            pass_on(t, 2)
            for d in (1, 3):
                arrived(t, d, 2)
                to_sib(t, d, 2)
                to_sib(t, 2, d)

        def stage_e(t):
            arrived(t, 2, 2)
            to_sib(t, 2, 2)

        def done(t):
            half = part(t, 0, 16)
            pltpu.make_async_copy(half, half, bsem.at[t]).wait()

        def drain(t):
            most = part(t, 0, 31)
            pltpu.make_async_copy(most, most, ssem.at[t]).wait()

        def run(stage):
            for t in range(chunks):
                stage(t)

        return run, (stage_a, stage_b, stage_c, stage_d, stage_e), done, drain

    mine = pl.ds(pl.multiple_of(8 * dom, 8), 8)
    run1, st1, done1, drain1 = gather_over_dom(gx, 4, rx, ssx, sib1, lambda t: xs.at[t, b])
    run2, st2, done2, drain2 = gather_over_dom(gp, 3, rp, ssp, sib2, lambda t: gp[t].at[mine])

    c_need = xchg(3, 0, need_v, need_r)
    run1(st1[0])
    h = pl.ds(0, 512), pl.ds(512, 512)
    c_a1 = [xchg(4, 0, a1.at[h[0]], a1o.at[h[0]]), xchg(5, 2, a1.at[h[1]], a1o.at[h[1]])]
    c_self = xchg(10, 1, xs.at[2 * b + 1 - c], sx.at[pl.ds(2 * c, 2)])
    c_w = [xchg(k, k, w, wg.at[q]) for k in range(3)]
    c_a2 = [
        xchg(6, 0, a2.at[h[0]], a2o.at[h[0]]), xchg(7, 2, a2.at[h[1]], a2o.at[h[1]]),
        xchg(8, 0, aq.at[h[0]], aqo.at[h[0]]), xchg(9, 2, aq.at[h[1]], aqo.at[h[1]]),
    ]
    for t in range(4):
        gx[t][mine] = xs[t, b]
    wg[q] = w[...]
    sx[pl.ds(2 * c, 2)] = xs[ts]

    c_need.wait_recv()
    to_smem = pltpu.make_async_copy(need_r, need_o, lsem)
    to_smem.start()
    to_smem.wait()

    for stage in st1[1:]:
        run1(stage)

    lists = (need_s, need_o)

    def pick(load, listed, row, dst):
        def body(p, _):
            halves = []
            for e in range(2):
                g = listed[row, 2 * p + e]
                v = load(lax.shift_right_logical(g, 1)).astype(F32)
                odd = (g & 1).astype(F32)
                halves.append(v[0:8] * (1.0 - odd) + v[8:16] * odd)
            dst[pl.ds(pl.multiple_of(p * 16, 16), 16), :] = jnp.concatenate(halves, 0).astype(BF)
            return 0

        lax.fori_loop(0, 32, body, 0)

    m32 = lane_groups(4, 32, 128)
    bases = (b * ROWS, (1 - b) * ROWS)
    ones = jnp.ones((WORDS, 128), BF)
    zero_bf, one_bf = jnp.zeros((), BF), jnp.ones((), BF)

    def hot(a, bit):
        return jnp.where(a == jnp.asarray(2.0 ** bit, BF), one_bf, zero_bf)

    for t in range(4):
        done1(t)
        for s in range(2):
            if t == 0 and s == 1:
                for cp in c_a1:
                    cp.wait_recv()
            adj = (a1, a1o)[s]
            pick(lambda i, t=t: gx[t][i], lists[s], 0, sel1)
            picked = sel1[...]
            for j in range(4):
                rhs1[j * WORDS : (j + 1) * WORDS, :] = picked * m32[j]

            def rows(i, _, t=t, s=s, adj=adj):
                a = adj[pl.ds(pl.multiple_of(i * RB, RB), RB), :]
                for j in range(4):
                    lhs[:, j * WORDS : (j + 1) * WORDS] = hot(a, 4 * t + j)
                part = dot(lhs[:, : 4 * WORDS], rhs1[...])
                at_rows = pl.ds(pl.multiple_of(bases[s] + i * RB, RB), RB)
                if t == 0:
                    acc1[at_rows, :] = part
                else:
                    acc1[at_rows, :] += part
                return 0

            lax.fori_loop(0, ROWS // RB, rows, 0)

    for s in range(2):
        adj = (a1, a1o)[s]

        def mean(i, _, s=s, adj=adj):
            a = adj[pl.ds(pl.multiple_of(i * RB, RB), RB), :]
            deg = dot(jnp.where(a != zero_bf, one_bf, zero_bf), ones)
            at_rows = pl.ds(pl.multiple_of(bases[s] + i * RB, RB), RB)
            x = acc1[at_rows, :]
            x = x + pltpu.roll(x, 32, 1)
            x = x + pltpu.roll(x, 64, 1)
            nr[at_rows, :] = x / jnp.maximum(deg, 1.0)
            return 0

        lax.fori_loop(0, ROWS // RB, mean, 0)

    lane = lax.broadcasted_iota(I32, (128, 128), 1)
    for t in range(4):
        x = nr[pl.ds(4 * t, 128, stride=16), :]
        for j in range(1, 4):
            x = jnp.where(lane >= 32 * j, nr[pl.ds(4 * t + j, 128, stride=16), :], x)
        npk[t] = x.astype(BF)
    c_near = [
        xchg(11 + e, e, npk.at[2 * rel[e][0] + rel[e][1]], ng.at[q]) for e in range(3)
    ]
    ng[q] = npk[ts]

    for cp in c_w:
        cp.wait_recv()
    for k in range(2):
        for cc in range(2):
            for bb in range(2):
                for qb in range(2):
                    piece = wg[2 * cc + bb, 64 * k + 32 * qb : 64 * k + 32 * qb + 32, :]
                    for j in range(4):
                        r0 = (2 * cc + qb) * 128 + j * 32
                        wr[k, r0 : r0 + 32, 128 * bb : 128 * bb + 128] = piece
    c_self.wait_recv()
    for cp in c_near:
        cp.wait_recv()
    for j in range(4):
        ls = jnp.concatenate([sx[i].reshape(128, 128) * m32[j] for i in range(4)], 1)
        ln = jnp.concatenate([ng[i] * m32[j] for i in range(4)], 1)
        hid[j] = jnp.maximum(dot(ls, wr[0]) + dot(ln, wr[1]), 0.0).astype(BF)

    low = lax.broadcasted_iota(I32, (256, 128), 1) < 64
    for k in range(2):
        for bb in range(2):
            r0 = 256 - 128 * k
            v = jnp.concatenate([wg[bb, r0 : r0 + 128, :], wg[2 + bb, r0 : r0 + 128, :]], 0)
            v = v.astype(F32)
            turned = pltpu.roll(v, 64, 1)
            for hh in range(2):
                fit, swap = (v, turned) if hh == 0 else (turned, v)
                wa = jnp.where(low, fit, 0.0).astype(BF)
                wb = jnp.where(low, 0.0, swap).astype(BF)
                for jj in range(2):
                    x = dot(hid[2 * jj], wa) + dot(hid[2 * jj + 1], wb)
                    pm[2 * bb + hh, 2 * k + jj] = x.astype(BF)
    c_p = [
        xchg(14 + e, e, pm.at[2 * rel[e][0] + rel[e][1], pl.ds(0, 2)], rg.at[ts, pl.ds(0, 2)])
        for e in range(3)
    ]
    c_q = [
        xchg(17 + e, e, pm.at[2 * rel[e][0] + rel[e][1], pl.ds(2, 2)], rg.at[ts, pl.ds(2, 2)])
        for e in range(3)
    ]
    rg[ts] = pm[ts]
    for cp in c_p:
        cp.wait_recv()
    for u in range(3):
        t0 = (0, 2, 5)[u]
        tiles = jnp.concatenate([rg[i // 2, i % 2] for i in range(t0, t0 + 3)], 1)
        l = lax.broadcasted_iota(I32, (384, 256), 1)
        r = lax.broadcasted_iota(I32, (384, 256), 0)
        j = quarter_of(l)
        goal = (5 * u + j) * 64 + l - CQ * j - 128 * t0
        x = dot(tiles, ones_at((r == goal) & (l < 5 * CQ))).astype(BF)
        for tile in range(2):
            gp[u][mine, tile] = x[:, 128 * tile : 128 * tile + 128].reshape(8, 16, 128)

    for stage in st2:
        run2(stage)

    for cp in c_q:
        cp.wait_recv()
    m64 = lane_groups(2, 64, 128)
    for i in range(16):
        rhsq[i * 128 : (i + 1) * 128, :] = rg[i // 4, 2 + (i % 4) // 2] * m64[i % 2]
    for cp in c_a2:
        cp.wait_recv()
    for s in range(2):
        own = (aq, aqo)[s]

        def own_rows(i, _, s=s, own=own):
            a = own[pl.ds(pl.multiple_of(i * RB, RB), RB), :]
            for j in range(16):
                lhs[:, j * 128 : (j + 1) * 128] = hot(a, j)
            accq[pl.ds(pl.multiple_of(s * ROWS + i * RB, RB), RB), :] = dot(lhs[:, :2048], rhsq[...])
            return 0

        lax.fori_loop(0, ROWS // RB, own_rows, 0)

    m43 = lane_groups(5, CQ, 256)
    for u in range(3):
        done2(u)
        for s in range(2):
            adj = (a2, a2o)[s]
            for tile in range(2):
                pick(lambda i, u=u, tile=tile: gp[u][i, tile], lists[s], 1, sel2.at[tile])
            picked = jnp.concatenate([sel2[0], sel2[1]], 1)
            for j in range(5):
                rhs2[j * WORDS : (j + 1) * WORDS, :] = picked * m43[j]

            def rows2(i, _, u=u, s=s, adj=adj):
                a = adj[pl.ds(pl.multiple_of(i * RB, RB), RB), :]
                for j in range(5):
                    lhs[:, j * WORDS : (j + 1) * WORDS] = hot(a, 5 * u + j)
                part = dot(lhs[...], rhs2[...])
                at_rows = pl.ds(pl.multiple_of(s * ROWS + i * RB, RB), RB)
                if u == 0:
                    acc2[at_rows, :] = part
                else:
                    acc2[at_rows, :] += part
                return 0

            lax.fori_loop(0, ROWS // RB, rows2, 0)

    l = lax.broadcasted_iota(I32, (256, 128), 0)
    m = lax.broadcasted_iota(I32, (256, 128), 1)
    cls = l - CQ * quarter_of(l)
    fold = [ones_at((m == cls + 64 * hh) & (l < 5 * CQ)) for hh in range(2)]
    fold = [jnp.concatenate([f, f], 0) for f in fold]
    low = lax.broadcasted_iota(I32, (RB, 128), 1) < 64
    for s in (1, 0):
        adj = (a2, a2o)[s]

        def close(i, _, s=s, adj=adj):
            res, own = [], []
            for hh in range(2):
                r0 = pl.multiple_of(512 * hh + i * RB, RB)
                a = adj[pl.ds(r0, RB), :]
                deg = dot(jnp.where(a != zero_bf, one_bf, zero_bf), ones)
                deg = jnp.maximum(deg, 1.0)
                at_rows = pl.ds(pl.multiple_of(s * ROWS + r0, RB), RB)
                x = acc2[at_rows, :] / jnp.concatenate([deg, deg], 1)
                top = x.astype(BF)
                rest = (x - top.astype(F32)).astype(BF)
                res.append(dot(jnp.concatenate([top, rest], 1), fold[hh]))
                y = accq[at_rows, :]
                own.append(y + pltpu.roll(y, 64, 1))
            total = res[0] + res[1] + jnp.where(low, own[0], own[1])
            lm[s, pl.ds(pl.multiple_of(i * RB, RB), RB), :] = total.astype(BF)
            return 0

        lax.fori_loop(0, 2, close, 0)
        if s == 1:
            c_l = [xchg(20, 0, lm.at[1], lgot.at[ts]), xchg(22, 2, lm.at[1], lgot.at[ts])]
    c_l.append(xchg(21, 1, lm.at[0], lgot.at[ts]))
    lgot[ts] = lm[0]
    for cp in c_l:
        cp.wait_recv()
    n = lax.broadcasted_iota(I32, (512, 256), 1)
    r = lax.broadcasted_iota(I32, (512, 256), 0)
    k = quarter_of(n)
    goal = 128 * k + n - CQ * k
    got = jnp.concatenate([lgot[i] for i in range(4)], 1)
    for hh in range(2):
        out[512 * hh : 512 * hh + 512, :] = dot(got, ones_at(r == goal + 64 * hh))[:, :172]

    for t in range(4):
        drain1(t)
    for t in range(3):
        drain2(t)
    for cp in started:
        cp.wait_send()


def per_device(
    features, self_weight1, neigh_weight1, need_first, count_first, adjacency_first,
    self_weight2, neigh_weight2, need_second, count_second, adjacency_second, seed_rows,
):
    xs = features.reshape(128, 4, 4, 2, 32).transpose(1, 3, 0, 2, 4).reshape(4, 2, 8, 16, 128)
    word = lax.broadcasted_iota(I32, (ROWS, WORDS), 1)
    a1 = jnp.where(word < 8 * count_first[0], adjacency_first, 0).astype(BF)
    a2 = jnp.where(word < 8 * count_second[0], adjacency_second, 0).astype(BF)
    own_word = lax.broadcasted_iota(I32, (ROWS, 128), 1)
    bit = jnp.left_shift(1, seed_rows % 16)
    aq = jnp.where(own_word == (seed_rows // 16)[:, None], bit[:, None], 0).astype(BF)
    needs = jnp.zeros((8, 128), I32).at[0, :64].set(need_first[0]).at[1, :64].set(need_second[0])

    def classes(x):
        return jnp.pad(x.reshape(128, 2, CQ), ((0, 0), (0, 0), (0, 64 - CQ))).reshape(128, 128)

    w = jnp.concatenate(
        [self_weight1, neigh_weight1, classes(self_weight2), classes(neigh_weight2)], 0
    )
    vm = pl.BlockSpec(memory_space=pltpu.VMEM)
    sm = pl.BlockSpec(memory_space=pltpu.SMEM)
    dma = pltpu.SemaphoreType.DMA
    return pl.pallas_call(
        kernel,
        out_shape=jax.ShapeDtypeStruct((ROWS, 172), F32),
        in_specs=[sm] + [vm] * 6,
        out_specs=vm,
        scratch_shapes=[
            *[pltpu.VMEM((256, 16, 128), BF)] * 4,
            *[pltpu.VMEM((256, 2, 16, 128), BF)] * 3,
            pltpu.VMEM((ROWS, WORDS), BF),
            pltpu.VMEM((ROWS, WORDS), BF),
            pltpu.VMEM((ROWS, 128), BF),
            pltpu.VMEM((4, 384, 128), BF),
            pltpu.VMEM((8, 128), I32),
            pltpu.SMEM((8, 128), I32),
            pltpu.VMEM((4, 8, 16, 128), BF),
            pltpu.VMEM((4, 128, 128), BF),
            pltpu.VMEM((4, 128, 128), BF),
            pltpu.VMEM((2 * ROWS, 128), F32),
            pltpu.VMEM((2 * ROWS, 128), F32),
            pltpu.VMEM((2 * ROWS, 256), F32),
            pltpu.VMEM((2 * ROWS, 128), F32),
            pltpu.VMEM((RB, 5 * WORDS), BF),
            pltpu.VMEM((4 * WORDS, 128), BF),
            pltpu.VMEM((5 * WORDS, 256), BF),
            pltpu.VMEM((2048, 128), BF),
            pltpu.VMEM((WORDS, 128), BF),
            pltpu.VMEM((2, WORDS, 128), BF),
            pltpu.VMEM((2, 512, 256), BF),
            pltpu.VMEM((4, 128, 256), BF),
            pltpu.VMEM((4, 4, 128, 128), BF),
            pltpu.VMEM((4, 4, 128, 128), BF),
            pltpu.VMEM((2, 512, 128), BF),
            pltpu.VMEM((4, 512, 128), BF),
            dma((4, 16)), dma((4,)), dma((4,)),
            dma((3, 16)), dma((3,)), dma((3,)),
            dma((23,)), dma((23,)), dma(()),
        ],
        compiler_params=pltpu.CompilerParams(
            collective_id=0, has_side_effects=True, vmem_limit_bytes=60 * 2**20
        ),
    )(needs, needs, xs, a1, a2, aq, w)


def solution(mesh):
    both = P(("dom", "batch"))
    rows = P(("dom", "batch"), None)
    wide = P("col", "batch")
    placed = (
        P("dom", "col"), wide, wide, rows, both, rows, wide, wide, rows, both, rows, both,
    )
    return jax.shard_map(
        per_device, mesh=mesh, in_specs=placed, out_specs=rows, check_vma=False
    )
```

```python
import jax
import jax.numpy as jnp
from jax import lax
from jax.experimental import pallas as pl
from jax.experimental.pallas import tpu as pltpu
from jax.sharding import PartitionSpec as P

MESH = pl.DeviceIdType.MESH
BF = jnp.bfloat16
F32 = jnp.float32
I32 = jnp.int32
ROWS = 1024
RB = 512
HB = 256
WORDS = 512
CQ = 43


def lane_groups(count, width, lanes):
    lane = lax.broadcasted_iota(I32, (1, lanes), 1)
    return [
        jnp.where((lane >= j * width) & (lane < (j + 1) * width), 1.0, 0.0).astype(BF)
        for j in range(count)
    ]


def quarter_of(index):
    return sum((index >= CQ * m).astype(I32) for m in range(1, 5))


def ones_at(hit):
    return jnp.where(hit, 1.0, 0.0).astype(BF)


def dot(a, b):
    return jnp.dot(a, b, preferred_element_type=F32)


def kernel(
    need1_s, need2_s, count1, count2, need1_v, need2_v, feats, w1s, w1n, w2s, w2n, seeds,
    adj1, adj2, out, xs, a1, a2, aq, w, raw1, raw2, fx, wt,
    gx0, gx1, gx2, gx3, gp0, gp1, gp2, a1o, a2o, aqo, wg, need1_r, need2_r, need1_o, need2_o, sx, npk, ng, acc1, nr, acc2, accq,
    lhs, rhs1, rhs2, rhsq, wr, hid, pm, rg, lm, lgot,
    rx, ssx, sib1, rp, ssp, sib2, mr, ms, lsem,
):
    gx, gp = (gx0, gx1, gx2, gx3), (gp0, gp1, gp2)
    dom = lax.axis_index("dom")
    b = lax.axis_index("batch")
    c = lax.axis_index("col")
    core = dom % 2
    s1, s2 = 2 + 6 * core, 8 - 6 * core
    p1, p2 = (dom // s1) % 4, (dom // s2) % 4

    def at(d1, d2):
        return dom + s1 * ((p1 + d1) % 4 - p1) + s2 * ((p2 + d2) % 4 - p2)

    sib = dom + 1 - 2 * core
    rel = [
        (1 - b, c, {"col": c, "batch": 1 - b}),
        (b, 1 - c, {"col": 1 - c, "batch": b}),
        (1 - b, 1 - c, {"col": 1 - c, "batch": 1 - b}),
    ]
    q = 2 * c + b
    ts = 2 * b + c

    load1 = pltpu.make_async_copy(adj1, raw1, lsem.at[0])
    load2 = pltpu.make_async_copy(adj2, raw2, lsem.at[1])
    load1.start()
    load2.start()
    barrier = pltpu.get_barrier_semaphore()
    for n in (at(1, 0), at(3, 0), at(0, 1), at(0, 3), sib):
        pl.semaphore_signal(barrier, inc=1, device_id={"dom": n}, device_id_type=MESH)
    for _, _, dev in rel:
        pl.semaphore_signal(barrier, inc=1, device_id=dev, device_id_type=MESH)
    for i in range(16):
        cut = slice(128 * i, 128 * i + 128)
        fx[cut, :64] = feats[:, cut].astype(F32).T
    lane = lax.broadcasted_iota(I32, (128, 128), 1)
    for t in range(4):
        parts = [fx[pl.ds(4 * t + j, 128, stride=16), :] for j in range(4)]
        for qb in range(2):
            x = parts[0] if qb == 0 else pltpu.roll(parts[0], 96, 1)
            for j in range(1, 4):
                turn = (32 * j - 32 * qb) % 128
                moved = pltpu.roll(parts[j], turn, 1) if turn else parts[j]
                x = jnp.where(lane >= 32 * j, moved, x)
            xs[t, qb] = x.astype(BF).reshape(8, 16, 128)
    pl.semaphore_wait(barrier, 8)

    started = []

    def xchg(k, e, src, dst):
        cp = pltpu.make_async_remote_copy(
            src_ref=src, dst_ref=dst, send_sem=ms.at[k], recv_sem=mr.at[k],
            device_id=rel[e][2], device_id_type=MESH,
        )
        cp.start()
        started.append(cp)
        return cp

    def gather_over_dom(g, chunks, rsem, ssem, bsem, own):
        def copy(t, src, target, rs, first=False):
            pltpu.make_async_remote_copy(
                src_ref=own(t) if first else part(t, src), dst_ref=part(t, src),
                send_sem=ssem.at[t], recv_sem=rs, device_id={"dom": target}, device_id_type=MESH,
            ).start()

        def part(t, src, count=1):
            return g[t].at[pl.ds(pl.multiple_of(8 * src, 8), 8 * count)]

        def slot(t, d1, d2):
            return rsem.at[t, 4 * d1 + d2]

        def arrived(t, d1, d2):
            pltpu.make_async_copy(part(t, 0), part(t, 0), slot(t, d1, d2)).wait()

        def to_sib(t, d1, d2):
            copy(t, at(d1, d2), sib, bsem.at[t])

        def spread(t, d1):
            copy(t, at(d1, 0), at(0, 1), slot(t, d1, 3))
            copy(t, at(d1, 0), at(0, 3), slot(t, d1, 1))

        def pass_on(t, d1):
            f = 3 - 2 * ((t + d1) % 2)
            copy(t, at(d1, f), at(0, 4 - f), slot(t, d1, 2))

        def stage_a(t):
            copy(t, dom, at(1, 0), slot(t, 3, 0), True)
            copy(t, dom, at(3, 0), slot(t, 1, 0), True)
            copy(t, dom, at(0, 1), slot(t, 0, 3), True)
            copy(t, dom, at(0, 3), slot(t, 0, 1), True)
            copy(t, dom, sib, bsem.at[t], True)

        def stage_b(t):
            for d1 in (1, 3):
                arrived(t, d1, 0)
                spread(t, d1)
            f = 3 - 2 * (t % 2)
            copy(t, at(f, 0), at(4 - f, 0), slot(t, 2, 0))
            for d2 in (1, 3):
                arrived(t, 0, d2)
            pass_on(t, 0)
            for d in (1, 3):
                to_sib(t, d, 0)
                to_sib(t, 0, d)

        def stage_c(t):
            arrived(t, 2, 0)
            spread(t, 2)
            for d1 in (1, 3):
                arrived(t, d1, 1)
                arrived(t, d1, 3)
                pass_on(t, d1)
            arrived(t, 0, 2)
            to_sib(t, 2, 0)
            to_sib(t, 0, 2)
            for d1 in (1, 3):
                to_sib(t, d1, 1)
                to_sib(t, d1, 3)

        def stage_d(t):
            arrived(t, 2, 1)
            arrived(t, 2, 3)
            pass_on(t, 2)
            for d in (1, 3):
                arrived(t, d, 2)
                to_sib(t, d, 2)
                to_sib(t, 2, d)

        def stage_e(t):
            arrived(t, 2, 2)
            to_sib(t, 2, 2)

        def done(t):
            half = part(t, 0, 16)
            pltpu.make_async_copy(half, half, bsem.at[t]).wait()

        def drain(t):
            most = part(t, 0, 31)
            pltpu.make_async_copy(most, most, ssem.at[t]).wait()

        stages = dict(a=stage_a, b=stage_b, c=stage_c, d=stage_d, e=stage_e, f=done)

        def run(order):
            for kind, t in zip(order[::2], order[1::2]):
                stages[kind](int(t))

        return run, drain

    mine = pl.ds(pl.multiple_of(8 * dom, 8), 8)
    run1, drain1 = gather_over_dom(gx, 4, rx, ssx, sib1, lambda t: xs.at[t, b])
    run2, drain2 = gather_over_dom(gp, 3, rp, ssp, sib2, lambda t: gp[t].at[mine])

    c_need = [xchg(3, 0, need1_v, need1_r), xchg(21, 0, need2_v, need2_r)]
    run1("a0a1a2a3")
    h = pl.ds(0, 512), pl.ds(512, 512)
    c_self = xchg(10, 1, xs.at[2 * b + 1 - c], sx.at[pl.ds(2 * c, 2)])

    def words(load, raw, count, dst):
        load.wait()
        word = lax.broadcasted_iota(I32, (128, WORDS), 1)
        limit = 8 * count[0]
        for i in range(8):
            cut = slice(128 * i, 128 * i + 128)
            dst[cut, :] = jnp.where(word < limit, raw[cut, :], 0).astype(F32).astype(BF)

    words(load1, raw1, count1, a1)
    c_a1 = [xchg(4, 0, a1.at[h[0]], a1o.at[h[0]]), xchg(5, 2, a1.at[h[1]], a1o.at[h[1]])]
    w[0:64] = w1s[...]
    w[64:128] = w1n[...]
    for k, x in enumerate((w2s, w2n)):
        wt[...] = jnp.zeros_like(wt)
        wt[0:CQ, :] = x[0:CQ, :].astype(F32)
        wt[64 : 64 + CQ, :] = x[CQ : 2 * CQ, :].astype(F32)
        w[128 + 128 * k : 256 + 128 * k] = wt[...].T.astype(BF)
    words(load2, raw2, count2, a2)
    row = lax.broadcasted_iota(I32, (128, 128), 0)
    for i in range(8):
        seed = seeds[i : i + 1, :]
        bit = jnp.left_shift(jnp.ones_like(seed), seed & 15)
        own = jnp.where(row == lax.shift_right_logical(seed, 4), bit, 0)
        aq[128 * i : 128 * i + 128, :] = own.astype(F32).T.astype(BF)
    c_w = [xchg(k, k, w, wg.at[q]) for k in range(3)]
    c_a2 = [
        xchg(6, 0, a2.at[h[0]], a2o.at[h[0]]), xchg(7, 2, a2.at[h[1]], a2o.at[h[1]]),
        xchg(8, 0, aq.at[h[0]], aqo.at[h[0]]), xchg(9, 2, aq.at[h[1]], aqo.at[h[1]]),
    ]
    for t in range(4):
        gx[t][mine] = xs[t, b]
    wg[q] = w[...]
    sx[pl.ds(2 * c, 2)] = xs[ts]

    rhs2[...] = jnp.zeros_like(rhs2)
    run1("b0b1b2b3c0c1c2c3d0d1e0f0")
    for cp in c_need:
        cp.wait_recv()
    to_smem = [
        pltpu.make_async_copy(need1_r, need1_o, lsem.at[2]),
        pltpu.make_async_copy(need2_r, need2_o, lsem.at[3]),
    ]
    for cp in to_smem:
        cp.start()
    for cp in to_smem:
        cp.wait()

    lists1, lists2 = (need1_s, need1_o), (need2_s, need2_o)

    def picked(load, listed, p):
        halves = []
        for e in range(2):
            g = listed[0, 2 * p + e]
            v = load(lax.shift_right_logical(g, 1)).astype(F32)
            odd = (g & 1).astype(F32)
            halves.append(v[0:8] * (1.0 - odd) + v[8:16] * odd)
        return jnp.concatenate(halves, 0).astype(BF)

    def word_rows(j, p):
        return pl.ds(pl.multiple_of(j * WORDS + p * 16, 16), 16)

    m32 = lane_groups(4, 32, 128)
    bases = (b * ROWS, (1 - b) * ROWS)
    ones = jnp.ones((WORDS, 128), BF)
    zero_bf, one_bf = jnp.zeros((), BF), jnp.ones((), BF)

    def hot(a, bit):
        return jnp.where(a == jnp.asarray(2.0 ** bit, BF), one_bf, zero_bf)

    def pick1(unit, k):
        t, sl = unit
        for i in range(8):
            p = 8 * k + i
            x = picked(lambda n: gx[t][n], lists1[sl], p)
            for j in range(4 if t < 3 else 3):
                rhs1[sl, word_rows(j, p), :] = x * m32[j]

    def loop(n, step):
        def body(k, _):
            step(k)
            return 0

        lax.fori_loop(0, n, body, 0)

    loop(4, lambda k: pick1((0, 0), k))
    units = [(t, sl) for t in range(4) for sl in range(2)]
    after = ["d2e1f1", "d3e2f2", "e3f3"] + [""] * 5
    for n, (t, sl) in enumerate(units):
        if n == 1:
            for cp in c_a1:
                cp.wait_recv()

        def rows(i, n=n, t=t, sl=sl):
            a = (a1, a1o)[sl][pl.ds(pl.multiple_of(i * RB, RB), RB), :]
            depth = WORDS * (4 if t < 3 else 3)
            for j in range(depth // WORDS):
                lhs[:, j * WORDS : (j + 1) * WORDS] = hot(a, 4 * t + j)
            if n < 7:
                for k in range(2):
                    pick1(units[n + 1], 2 * i + k)
            part = dot(lhs[:, :depth], rhs1[sl, :depth, :])
            at_rows = pl.ds(pl.multiple_of(bases[sl] + i * RB, RB), RB)
            if t == 0:
                acc1[at_rows, :] = part
            else:
                acc1[at_rows, :] += part

        loop(2, rows)
        run1(after[n])

    for s in range(2):
        adj = (a1, a1o)[s]

        def mean(i, _, s=s, adj=adj):
            a = adj[pl.ds(pl.multiple_of(i * RB, RB), RB), :]
            deg = dot(jnp.where(a != zero_bf, one_bf, zero_bf), ones)
            at_rows = pl.ds(pl.multiple_of(bases[s] + i * RB, RB), RB)
            x = acc1[at_rows, :]
            x = x + pltpu.roll(x, 32, 1)
            x = x + pltpu.roll(x, 64, 1)
            nr[at_rows, :] = x / jnp.maximum(deg, 1.0)
            return 0

        lax.fori_loop(0, ROWS // RB, mean, 0)

    lane = lax.broadcasted_iota(I32, (128, 128), 1)
    for t in range(4):
        x = nr[pl.ds(4 * t, 128, stride=16), :]
        for j in range(1, 4):
            x = jnp.where(lane >= 32 * j, nr[pl.ds(4 * t + j, 128, stride=16), :], x)
        npk[t] = x.astype(BF)
    c_near = [
        xchg(11 + e, e, npk.at[2 * rel[e][0] + rel[e][1]], ng.at[q]) for e in range(3)
    ]
    ng[q] = npk[ts]

    for cp in c_w:
        cp.wait_recv()
    for k in range(2):
        for cc in range(2):
            for bb in range(2):
                for qb in range(2):
                    piece = wg[2 * cc + bb, 64 * k + 32 * qb : 64 * k + 32 * qb + 32, :]
                    for j in range(4):
                        r0 = (2 * cc + qb) * 128 + j * 32
                        wr[k, r0 : r0 + 32, 128 * bb : 128 * bb + 128] = piece
    c_self.wait_recv()
    for cp in c_near:
        cp.wait_recv()
    for j in range(4):
        ls = jnp.concatenate([sx[i].reshape(128, 128) * m32[j] for i in range(4)], 1)
        ln = jnp.concatenate([ng[i] * m32[j] for i in range(4)], 1)
        hid[j] = jnp.maximum(dot(ls, wr[0]) + dot(ln, wr[1]), 0.0).astype(BF)

    low = lax.broadcasted_iota(I32, (256, 128), 1) < 64
    for k in range(2):
        for bb in range(2):
            r0 = 256 - 128 * k
            v = jnp.concatenate([wg[bb, r0 : r0 + 128, :], wg[2 + bb, r0 : r0 + 128, :]], 0)
            v = v.astype(F32)
            turned = pltpu.roll(v, 64, 1)
            for hh in range(2):
                fit, swap = (v, turned) if hh == 0 else (turned, v)
                wa = jnp.where(low, fit, 0.0).astype(BF)
                wb = jnp.where(low, 0.0, swap).astype(BF)
                for jj in range(2):
                    x = dot(hid[2 * jj], wa) + dot(hid[2 * jj + 1], wb)
                    pm[2 * bb + hh, 2 * k + jj] = x.astype(BF)
    c_p = [
        xchg(14 + e, e, pm.at[2 * rel[e][0] + rel[e][1], pl.ds(0, 2)], rg.at[ts, pl.ds(0, 2)])
        for e in range(3)
    ]
    c_q = [
        xchg(17 + e, e, pm.at[2 * rel[e][0] + rel[e][1], pl.ds(2, 2)], rg.at[ts, pl.ds(2, 2)])
        for e in range(3)
    ]
    rg[ts] = pm[ts]
    for cp in c_p:
        cp.wait_recv()
    for u in range(3):
        t0 = (0, 2, 5)[u]
        tiles = jnp.concatenate([rg[i // 2, i % 2] for i in range(t0, t0 + 3)], 1)
        l = lax.broadcasted_iota(I32, (384, 256), 1)
        r = lax.broadcasted_iota(I32, (384, 256), 0)
        j = quarter_of(l)
        goal = (5 * u + j) * 64 + l - CQ * j - 128 * t0
        x = dot(tiles, ones_at((r == goal) & (l < 5 * CQ))).astype(BF)
        for tile in range(2):
            gp[u][mine, tile] = x[:, 128 * tile : 128 * tile + 128].reshape(8, 16, 128)

    run2("a0a1a2b0b1b2")

    for cp in c_q:
        cp.wait_recv()
    m64 = lane_groups(2, 64, 128)
    for i in range(16):
        rhsq[i * 128 : (i + 1) * 128, :] = rg[i // 4, 2 + (i % 4) // 2] * m64[i % 2]
    for cp in c_a2:
        cp.wait_recv()
    for s in range(2):
        own = (aq, aqo)[s]

        def own_rows(i, _, s=s, own=own):
            a = own[pl.ds(pl.multiple_of(i * RB, RB), RB), :]
            for j in range(16):
                lhs[:, j * 128 : (j + 1) * 128] = hot(a, j)
            accq[pl.ds(pl.multiple_of(s * ROWS + i * RB, RB), RB), :] = dot(lhs[:, :2048], rhsq[...])
            return 0

        lax.fori_loop(0, ROWS // RB, own_rows, 0)
        run2("c0c1" if s == 0 else "c2d0e0d1f0")

    m43 = lane_groups(5, CQ, 256)
    def pick2(unit, k):
        u, sl = unit
        for i in range(8):
            p = 8 * k + i
            for tile in range(2):
                x = picked(lambda n: gp[u][n, tile], lists2[sl], p)
                cut = slice(128 * tile, 128 * tile + 128)
                for j in range(2 * tile, 2 * tile + 3):
                    rhs2[sl, word_rows(j, p), cut] = x * m43[j][:, cut]

    loop(4, lambda k: pick2((0, 0), k))
    units2 = [(u, sl) for u in range(3) for sl in range(2)]
    after = ["d2e1f1", "", "e2f2"] + [""] * 3
    for n, (u, sl) in enumerate(units2):

        def rows2(i, n=n, u=u, sl=sl):
            a = (a2, a2o)[sl][pl.ds(pl.multiple_of(i * RB, RB), RB), :]
            for j in range(5):
                lhs[:, j * WORDS : (j + 1) * WORDS] = hot(a, 5 * u + j)
            if n < 5:
                for k in range(2):
                    pick2(units2[n + 1], 2 * i + k)
            part = dot(lhs[...], rhs2[sl])
            at_rows = pl.ds(pl.multiple_of(sl * ROWS + i * RB, RB), RB)
            if u == 0:
                acc2[at_rows, :] = part
            else:
                acc2[at_rows, :] += part

        loop(2, rows2)
        run2(after[n])

    l = lax.broadcasted_iota(I32, (48, 256), 1)
    m = lax.broadcasted_iota(I32, (48, 256), 0)
    fold = ones_at((m == l - CQ * quarter_of(l)) & (l < 5 * CQ))
    fold_own = ones_at((m == (l & 63)) & (m < CQ))
    fold = jnp.concatenate([fold, fold, fold_own], 1)
    c_l = []
    for s in (1, 0):
        adj = (a2, a2o)[s]

        def split(x):
            top = x.astype(BF)
            return [top, (x - top.astype(F32)).astype(BF)]

        for i in range(4):
            a = adj[HB * i : HB * i + HB, :]
            deg = dot(jnp.where(a != zero_bf, one_bf, zero_bf), ones)
            deg = jnp.maximum(deg, 1.0)
            at_rows = slice(s * ROWS + HB * i, s * ROWS + HB * i + HB)
            x = acc2[at_rows, :] / jnp.concatenate([deg, deg], 1)
            all_of = jnp.concatenate(split(x) + split(accq[at_rows, :]), 1)
            lm[s, :, HB * i : HB * i + HB] = lax.dot_general(
                fold, all_of, (((1,), (1,)), ((), ())), preferred_element_type=F32
            ).astype(BF)
        if s == 1:
            c_l = [xchg(20, 0, lm.at[1], lgot.at[ts]), xchg(22, 2, lm.at[1], lgot.at[ts])]
    c_l.append(xchg(23, 1, lm.at[0], lgot.at[ts]))
    lgot[ts] = lm[0]
    for cp in c_l:
        cp.wait_recv()
    for k in range(4):
        out[CQ * k : CQ * k + CQ, :] = lgot[k, 0:CQ, :].astype(F32)

    for t in range(4):
        drain1(t)
    for t in range(3):
        drain2(t)
    for cp in started:
        cp.wait_send()


def per_device(
    features, self_weight1, neigh_weight1, need_first, count_first, adjacency_first,
    self_weight2, neigh_weight2, need_second, count_second, adjacency_second, seed_rows,
):
    vm = pl.BlockSpec(memory_space=pltpu.VMEM)
    sm = pl.BlockSpec(memory_space=pltpu.SMEM)
    dma = pltpu.SemaphoreType.DMA
    logits = pl.pallas_call(
        kernel,
        out_shape=jax.ShapeDtypeStruct((172, ROWS), F32),
        in_specs=[sm] * 4 + [vm] * 8 + [pl.BlockSpec(memory_space=pl.ANY)] * 2,
        out_specs=vm,
        scratch_shapes=[
            pltpu.VMEM((4, 2, 8, 16, 128), BF),
            pltpu.VMEM((ROWS, WORDS), BF),
            pltpu.VMEM((ROWS, WORDS), BF),
            pltpu.VMEM((ROWS, 128), BF),
            pltpu.VMEM((384, 128), BF),
            pltpu.VMEM((ROWS, WORDS), I32),
            pltpu.VMEM((ROWS, WORDS), I32),
            pltpu.VMEM((2048, 128), F32),
            pltpu.VMEM((128, 128), F32),
            *[pltpu.VMEM((256, 16, 128), BF)] * 4,
            *[pltpu.VMEM((256, 2, 16, 128), BF)] * 3,
            pltpu.VMEM((ROWS, WORDS), BF),
            pltpu.VMEM((ROWS, WORDS), BF),
            pltpu.VMEM((ROWS, 128), BF),
            pltpu.VMEM((4, 384, 128), BF),
            pltpu.VMEM((1, 64), I32),
            pltpu.VMEM((1, 64), I32),
            pltpu.SMEM((1, 64), I32),
            pltpu.SMEM((1, 64), I32),
            pltpu.VMEM((4, 8, 16, 128), BF),
            pltpu.VMEM((4, 128, 128), BF),
            pltpu.VMEM((4, 128, 128), BF),
            pltpu.VMEM((2 * ROWS, 128), F32),
            pltpu.VMEM((2 * ROWS, 128), F32),
            pltpu.VMEM((2 * ROWS, 256), F32),
            pltpu.VMEM((2 * ROWS, 128), F32),
            pltpu.VMEM((RB, 5 * WORDS), BF),
            pltpu.VMEM((2, 4 * WORDS, 128), BF),
            pltpu.VMEM((2, 5 * WORDS, 256), BF),
            pltpu.VMEM((2048, 128), BF),
            pltpu.VMEM((2, 512, 256), BF),
            pltpu.VMEM((4, 128, 256), BF),
            pltpu.VMEM((4, 4, 128, 128), BF),
            pltpu.VMEM((4, 4, 128, 128), BF),
            pltpu.VMEM((2, 48, ROWS), BF),
            pltpu.VMEM((4, 48, ROWS), BF),
            dma((4, 16)), dma((4,)), dma((4,)),
            dma((3, 16)), dma((3,)), dma((3,)),
            dma((24,)), dma((24,)), dma((4,)),
        ],
        compiler_params=pltpu.CompilerParams(
            collective_id=0, has_side_effects=True, vmem_limit_bytes=60 * 2**20
        ),
    )(
        need_first, need_second, count_first, count_second, need_first, need_second,
        features.T, self_weight1, neigh_weight1, self_weight2.T, neigh_weight2.T,
        seed_rows.reshape(8, 128), adjacency_first, adjacency_second,
    )
    return logits.T


def solution(mesh):
    both = P(("dom", "batch"))
    rows = P(("dom", "batch"), None)
    wide = P("col", "batch")
    placed = (
        P("dom", "col"), wide, wide, rows, both, rows, wide, wide, rows, both, rows, both,
    )
    return jax.shard_map(
        per_device, mesh=mesh, in_specs=placed, out_specs=rows, check_vma=False
    )
```

```python
import jax
import jax.numpy as jnp
from jax import lax
from jax.experimental import pallas as pl
from jax.experimental.pallas import tpu as pltpu
from jax.sharding import PartitionSpec as P

MESH = pl.DeviceIdType.MESH
BF = jnp.bfloat16
F32 = jnp.float32
I32 = jnp.int32
ROWS = 1024
RB = 512
HB = 256
WORDS = 512
CQ = 43


def lane_groups(count, width, lanes):
    lane = lax.broadcasted_iota(I32, (1, lanes), 1)
    return [
        jnp.where((lane >= j * width) & (lane < (j + 1) * width), 1.0, 0.0).astype(BF)
        for j in range(count)
    ]


def quarter_of(index):
    return sum((index >= CQ * m).astype(I32) for m in range(1, 5))


def ones_at(hit):
    return jnp.where(hit, 1.0, 0.0).astype(BF)


def dot(a, b):
    return jnp.dot(a, b, preferred_element_type=F32)


def kernel(
    need1_s, need2_s, count1, count2, need1_v, need2_v, feats, w1s, w1n, w2s, w2n, seeds,
    adj1, adj2, out, xs, a1, a2, aq, w, raw1, raw2, fx, wt,
    gx0, gx1, gx2, gx3, gp0, gp1, gp2, a1o, a2o, aqo, wg, need1_r, need2_r, need1_o, need2_o, sx, npk, ng, acc1, nr, acc2, accq,
    lhs, rhs1, rhs2, rhsq, wr, hid, pm, rg, lm, lgot,
    rx, ssx, sib1, rp, ssp, sib2, mr, ms, lsem,
):
    gx, gp = (gx0, gx1, gx2, gx3), (gp0, gp1, gp2)
    dom = lax.axis_index("dom")
    b = lax.axis_index("batch")
    c = lax.axis_index("col")
    core = dom % 2
    s1, s2 = 2 + 6 * core, 8 - 6 * core
    p1, p2 = (dom // s1) % 4, (dom // s2) % 4

    def at(d1, d2):
        return dom + s1 * ((p1 + d1) % 4 - p1) + s2 * ((p2 + d2) % 4 - p2)

    sib = dom + 1 - 2 * core
    rel = [
        (1 - b, c, {"col": c, "batch": 1 - b}),
        (b, 1 - c, {"col": 1 - c, "batch": b}),
        (1 - b, 1 - c, {"col": 1 - c, "batch": 1 - b}),
    ]
    q = 2 * c + b
    ts = 2 * b + c

    load1 = pltpu.make_async_copy(adj1, raw1, lsem.at[0])
    load2 = pltpu.make_async_copy(adj2, raw2, lsem.at[1])
    load1.start()
    load2.start()
    barrier = pltpu.get_barrier_semaphore()
    for n in (at(1, 0), at(3, 0), at(0, 1), at(0, 3), sib):
        pl.semaphore_signal(barrier, inc=1, device_id={"dom": n}, device_id_type=MESH)
    for _, _, dev in rel:
        pl.semaphore_signal(barrier, inc=1, device_id=dev, device_id_type=MESH)
    for i in range(16):
        cut = slice(128 * i, 128 * i + 128)
        fx[cut, :64] = feats[:, cut].astype(F32).T
    lane = lax.broadcasted_iota(I32, (128, 128), 1)
    for t in range(4):
        parts = [fx[pl.ds(4 * t + j, 128, stride=16), :] for j in range(4)]
        for qb in range(2):
            x = parts[0] if qb == 0 else pltpu.roll(parts[0], 96, 1)
            for j in range(1, 4):
                turn = (32 * j - 32 * qb) % 128
                moved = pltpu.roll(parts[j], turn, 1) if turn else parts[j]
                x = jnp.where(lane >= 32 * j, moved, x)
            xs[t, qb] = x.astype(BF).reshape(8, 16, 128)
    pl.semaphore_wait(barrier, 8)

    started = []

    def xchg(k, e, src, dst):
        cp = pltpu.make_async_remote_copy(
            src_ref=src, dst_ref=dst, send_sem=ms.at[k], recv_sem=mr.at[k],
            device_id=rel[e][2], device_id_type=MESH,
        )
        cp.start()
        started.append(cp)
        return cp

    def gather_over_dom(g, chunks, rsem, ssem, bsem, own):
        def copy(t, src, target, rs, first=False):
            pltpu.make_async_remote_copy(
                src_ref=own(t) if first else part(t, src), dst_ref=part(t, src),
                send_sem=ssem.at[t], recv_sem=rs, device_id={"dom": target}, device_id_type=MESH,
            ).start()

        def part(t, src, count=1):
            return g[t].at[pl.ds(pl.multiple_of(8 * src, 8), 8 * count)]

        def slot(t, d1, d2):
            return rsem.at[t, 4 * d1 + d2]

        def arrived(t, d1, d2):
            pltpu.make_async_copy(part(t, 0), part(t, 0), slot(t, d1, d2)).wait()

        def to_sib(t, d1, d2):
            copy(t, at(d1, d2), sib, bsem.at[t])

        def spread(t, d1):
            copy(t, at(d1, 0), at(0, 1), slot(t, d1, 3))
            copy(t, at(d1, 0), at(0, 3), slot(t, d1, 1))

        def pass_on(t, d1):
            f = 3 - 2 * ((t + d1) % 2)
            copy(t, at(d1, f), at(0, 4 - f), slot(t, d1, 2))

        def stage_a(t):
            copy(t, dom, at(1, 0), slot(t, 3, 0), True)
            copy(t, dom, at(3, 0), slot(t, 1, 0), True)
            copy(t, dom, at(0, 1), slot(t, 0, 3), True)
            copy(t, dom, at(0, 3), slot(t, 0, 1), True)
            copy(t, dom, sib, bsem.at[t], True)

        def stage_b(t):
            for d1 in (1, 3):
                arrived(t, d1, 0)
                spread(t, d1)
            f = 3 - 2 * (t % 2)
            copy(t, at(f, 0), at(4 - f, 0), slot(t, 2, 0))
            for d2 in (1, 3):
                arrived(t, 0, d2)
            pass_on(t, 0)
            for d in (1, 3):
                to_sib(t, d, 0)
                to_sib(t, 0, d)

        def stage_c(t):
            arrived(t, 2, 0)
            spread(t, 2)
            for d1 in (1, 3):
                arrived(t, d1, 1)
                arrived(t, d1, 3)
                pass_on(t, d1)
            arrived(t, 0, 2)
            to_sib(t, 2, 0)
            to_sib(t, 0, 2)
            for d1 in (1, 3):
                to_sib(t, d1, 1)
                to_sib(t, d1, 3)

        def stage_d(t):
            arrived(t, 2, 1)
            arrived(t, 2, 3)
            pass_on(t, 2)
            for d in (1, 3):
                arrived(t, d, 2)
                to_sib(t, d, 2)
                to_sib(t, 2, d)

        def stage_e(t):
            arrived(t, 2, 2)
            to_sib(t, 2, 2)

        def done(t):
            half = part(t, 0, 16)
            pltpu.make_async_copy(half, half, bsem.at[t]).wait()

        def drain(t):
            most = part(t, 0, 31)
            pltpu.make_async_copy(most, most, ssem.at[t]).wait()

        stages = dict(a=stage_a, b=stage_b, c=stage_c, d=stage_d, e=stage_e, f=done)

        def run(order):
            for kind, t in zip(order[::2], order[1::2]):
                stages[kind](int(t))

        return run, drain

    mine = pl.ds(pl.multiple_of(8 * dom, 8), 8)
    run1, drain1 = gather_over_dom(gx, 4, rx, ssx, sib1, lambda t: xs.at[t, b])
    run2, drain2 = gather_over_dom(gp, 3, rp, ssp, sib2, lambda t: gp[t].at[mine])

    c_need = [xchg(3, 0, need1_v, need1_r), xchg(21, 0, need2_v, need2_r)]
    run1("a0a1a2a3")
    h = pl.ds(0, 512), pl.ds(512, 512)
    c_self = xchg(10, 1, xs.at[2 * b + 1 - c], sx.at[pl.ds(2 * c, 2)])

    def words(load, raw, count, dst):
        load.wait()
        word = lax.broadcasted_iota(I32, (128, WORDS), 1)
        limit = 8 * count[0]
        for i in range(8):
            cut = slice(128 * i, 128 * i + 128)
            dst[cut, :] = jnp.where(word < limit, raw[cut, :], 0).astype(F32).astype(BF)

    words(load1, raw1, count1, a1)
    c_a1 = [xchg(4, 0, a1.at[h[0]], a1o.at[h[0]]), xchg(5, 2, a1.at[h[1]], a1o.at[h[1]])]
    w[0:64] = w1s[...]
    w[64:128] = w1n[...]
    for k, x in enumerate((w2s, w2n)):
        wt[...] = jnp.zeros_like(wt)
        wt[0:CQ, :] = x[0:CQ, :].astype(F32)
        wt[64 : 64 + CQ, :] = x[CQ : 2 * CQ, :].astype(F32)
        w[128 + 128 * k : 256 + 128 * k] = wt[...].T.astype(BF)
    words(load2, raw2, count2, a2)
    row = lax.broadcasted_iota(I32, (128, 128), 0)
    for i in range(8):
        seed = seeds[i : i + 1, :]
        bit = jnp.left_shift(jnp.ones_like(seed), seed & 15)
        own = jnp.where(row == lax.shift_right_logical(seed, 4), bit, 0)
        aq[128 * i : 128 * i + 128, :] = own.astype(F32).T.astype(BF)
    c_w = [xchg(k, k, w, wg.at[q]) for k in range(3)]
    c_a2 = [
        xchg(6, 0, a2.at[h[0]], a2o.at[h[0]]), xchg(7, 2, a2.at[h[1]], a2o.at[h[1]]),
        xchg(8, 0, aq.at[h[0]], aqo.at[h[0]]), xchg(9, 2, aq.at[h[1]], aqo.at[h[1]]),
    ]
    for t in range(4):
        gx[t][mine] = xs[t, b]
    wg[q] = w[...]
    sx[pl.ds(2 * c, 2)] = xs[ts]

    rhs2[...] = jnp.zeros_like(rhs2)
    run1("b0b1b2b3c0c1c2c3d0d1e0d2e1f0")
    for cp in c_need:
        cp.wait_recv()
    to_smem = [
        pltpu.make_async_copy(need1_r, need1_o, lsem.at[2]),
        pltpu.make_async_copy(need2_r, need2_o, lsem.at[3]),
    ]
    for cp in to_smem:
        cp.start()
    for cp in to_smem:
        cp.wait()

    lists1, lists2 = (need1_s, need1_o), (need2_s, need2_o)

    def picked(load, listed, p):
        halves = []
        for e in range(2):
            g = listed[0, 2 * p + e]
            v = load(lax.shift_right_logical(g, 1)).astype(F32)
            odd = (g & 1).astype(F32)
            halves.append(v[0:8] * (1.0 - odd) + v[8:16] * odd)
        return jnp.concatenate(halves, 0).astype(BF)

    def word_rows(j, p):
        return pl.ds(pl.multiple_of(j * WORDS + p * 16, 16), 16)

    m32 = lane_groups(4, 32, 128)
    bases = (b * ROWS, (1 - b) * ROWS)
    ones = jnp.ones((WORDS, 128), BF)
    zero_bf, one_bf = jnp.zeros((), BF), jnp.ones((), BF)

    def hot(a, bit):
        return jnp.where(a == jnp.asarray(2.0 ** bit, BF), one_bf, zero_bf)

    def pick1(unit, k):
        t, sl = unit
        for i in range(8):
            p = 8 * k + i
            x = picked(lambda n: gx[t][n], lists1[sl], p)
            for j in range(4 if t < 3 else 3):
                rhs1[sl, word_rows(j, p), :] = x * m32[j]

    def loop(n, step):
        def body(k, _):
            step(k)
            return 0

        lax.fori_loop(0, n, body, 0)

    loop(4, lambda k: pick1((0, 0), k))
    units = [(t, sl) for t in range(4) for sl in range(2)]
    after = ["d3e2f1", "e3f2", "f3"] + [""] * 5
    for n, (t, sl) in enumerate(units):
        if n == 1:
            for cp in c_a1:
                cp.wait_recv()

        def rows(i, n=n, t=t, sl=sl):
            a = (a1, a1o)[sl][pl.ds(pl.multiple_of(i * RB, RB), RB), :]
            depth = WORDS * (4 if t < 3 else 3)
            for j in range(depth // WORDS):
                lhs[:, j * WORDS : (j + 1) * WORDS] = hot(a, 4 * t + j)
            if n < 7:
                for k in range(2):
                    pick1(units[n + 1], 2 * i + k)
            part = dot(lhs[:, :depth], rhs1[sl, :depth, :])
            at_rows = pl.ds(pl.multiple_of(bases[sl] + i * RB, RB), RB)
            if t == 0:
                acc1[at_rows, :] = part
            else:
                acc1[at_rows, :] += part

        loop(2, rows)
        run1(after[n])

    for s in range(2):
        adj = (a1, a1o)[s]

        def mean(i, _, s=s, adj=adj):
            a = adj[pl.ds(pl.multiple_of(i * RB, RB), RB), :]
            deg = dot(jnp.where(a != zero_bf, one_bf, zero_bf), ones)
            at_rows = pl.ds(pl.multiple_of(bases[s] + i * RB, RB), RB)
            x = acc1[at_rows, :]
            x = x + pltpu.roll(x, 32, 1)
            x = x + pltpu.roll(x, 64, 1)
            nr[at_rows, :] = x / jnp.maximum(deg, 1.0)
            return 0

        lax.fori_loop(0, ROWS // RB, mean, 0)

    lane = lax.broadcasted_iota(I32, (128, 128), 1)
    for t in range(4):
        x = nr[pl.ds(4 * t, 128, stride=16), :]
        for j in range(1, 4):
            x = jnp.where(lane >= 32 * j, nr[pl.ds(4 * t + j, 128, stride=16), :], x)
        npk[t] = x.astype(BF)
    c_near = [
        xchg(11 + e, e, npk.at[2 * rel[e][0] + rel[e][1]], ng.at[q]) for e in range(3)
    ]
    ng[q] = npk[ts]

    for cp in c_w:
        cp.wait_recv()
    for k in range(2):
        for cc in range(2):
            for bb in range(2):
                for qb in range(2):
                    piece = wg[2 * cc + bb, 64 * k + 32 * qb : 64 * k + 32 * qb + 32, :]
                    for j in range(4):
                        r0 = (2 * cc + qb) * 128 + j * 32
                        wr[k, r0 : r0 + 32, 128 * bb : 128 * bb + 128] = piece
    c_self.wait_recv()
    for cp in c_near:
        cp.wait_recv()
    for j in range(4):
        ls = jnp.concatenate([sx[i].reshape(128, 128) * m32[j] for i in range(4)], 1)
        ln = jnp.concatenate([ng[i] * m32[j] for i in range(4)], 1)
        hid[j] = jnp.maximum(dot(ls, wr[0]) + dot(ln, wr[1]), 0.0).astype(BF)

    low = lax.broadcasted_iota(I32, (256, 128), 1) < 64
    for k in range(2):
        for bb in range(2):
            r0 = 256 - 128 * k
            v = jnp.concatenate([wg[bb, r0 : r0 + 128, :], wg[2 + bb, r0 : r0 + 128, :]], 0)
            v = v.astype(F32)
            turned = pltpu.roll(v, 64, 1)
            for hh in range(2):
                fit, swap = (v, turned) if hh == 0 else (turned, v)
                wa = jnp.where(low, fit, 0.0).astype(BF)
                wb = jnp.where(low, 0.0, swap).astype(BF)
                for jj in range(2):
                    x = dot(hid[2 * jj], wa) + dot(hid[2 * jj + 1], wb)
                    pm[2 * bb + hh, 2 * k + jj] = x.astype(BF)
    c_p = [
        xchg(14 + e, e, pm.at[2 * rel[e][0] + rel[e][1], pl.ds(0, 2)], rg.at[ts, pl.ds(0, 2)])
        for e in range(3)
    ]
    c_q = [
        xchg(17 + e, e, pm.at[2 * rel[e][0] + rel[e][1], pl.ds(2, 2)], rg.at[ts, pl.ds(2, 2)])
        for e in range(3)
    ]
    rg[ts] = pm[ts]
    for cp in c_p:
        cp.wait_recv()
    for u in range(3):
        t0 = (0, 2, 5)[u]
        tiles = jnp.concatenate([rg[i // 2, i % 2] for i in range(t0, t0 + 3)], 1)
        l = lax.broadcasted_iota(I32, (384, 256), 1)
        r = lax.broadcasted_iota(I32, (384, 256), 0)
        j = quarter_of(l)
        goal = (5 * u + j) * 64 + l - CQ * j - 128 * t0
        x = dot(tiles, ones_at((r == goal) & (l < 5 * CQ))).astype(BF)
        for tile in range(2):
            gp[u][mine, tile] = x[:, 128 * tile : 128 * tile + 128].reshape(8, 16, 128)

    run2("a0a1a2b0b1b2")

    for cp in c_q:
        cp.wait_recv()
    m64 = lane_groups(2, 64, 128)
    for i in range(16):
        rhsq[i * 128 : (i + 1) * 128, :] = rg[i // 4, 2 + (i % 4) // 2] * m64[i % 2]
    for cp in c_a2:
        cp.wait_recv()
    for s in range(2):
        own = (aq, aqo)[s]

        def own_rows(i, _, s=s, own=own):
            a = own[pl.ds(pl.multiple_of(i * RB, RB), RB), :]
            for j in range(16):
                lhs[:, j * 128 : (j + 1) * 128] = hot(a, j)
            accq[pl.ds(pl.multiple_of(s * ROWS + i * RB, RB), RB), :] = dot(lhs[:, :2048], rhsq[...])
            return 0

        lax.fori_loop(0, ROWS // RB, own_rows, 0)
        run2("c0c1" if s == 0 else "c2d0d1e0d2e1f0")

    m43 = lane_groups(5, CQ, 256)
    l = lax.broadcasted_iota(I32, (48, 256), 1)
    m = lax.broadcasted_iota(I32, (48, 256), 0)
    fold = ones_at((m == l - CQ * quarter_of(l)) & (l < 5 * CQ))
    fold_own = ones_at((m == (l & 63)) & (m < CQ))
    fold = jnp.concatenate([fold, fold, fold_own], 1)

    def split(x):
        top = x.astype(BF)
        return [top, (x - top.astype(F32)).astype(BF)]

    def close(sl, i):
        a = (a2, a2o)[sl][HB * i : HB * i + HB, :]
        deg = dot(jnp.where(a != zero_bf, one_bf, zero_bf), ones)
        deg = jnp.maximum(deg, 1.0)
        at_rows = slice(sl * ROWS + HB * i, sl * ROWS + HB * i + HB)
        x = acc2[at_rows, :] / jnp.concatenate([deg, deg], 1)
        all_of = jnp.concatenate(split(x) + split(accq[at_rows, :]), 1)
        lm[sl, :, HB * i : HB * i + HB] = lax.dot_general(
            fold, all_of, (((1,), (1,)), ((), ())), preferred_element_type=F32
        ).astype(BF)

    def pick2(unit, k):
        u, sl = unit
        for i in range(8):
            p = 8 * k + i
            for tile in range(2):
                x = picked(lambda n: gp[u][n, tile], lists2[sl], p)
                cut = slice(128 * tile, 128 * tile + 128)
                for j in range(2 * tile, 2 * tile + 3):
                    rhs2[sl, word_rows(j, p), cut] = x * m43[j][:, cut]

    loop(4, lambda k: pick2((0, 0), k))
    units2 = [(u, sl) for u in range(3) for sl in range(2)]
    after = ["e2f1", "", "f2"] + [""] * 3
    for n, (u, sl) in enumerate(units2):

        def rows2(i, n=n, u=u, sl=sl):
            a = (a2, a2o)[sl][pl.ds(pl.multiple_of(i * RB, RB), RB), :]
            for j in range(5):
                lhs[:, j * WORDS : (j + 1) * WORDS] = hot(a, 5 * u + j)
            if n < 5:
                for k in range(2):
                    pick2(units2[n + 1], 2 * i + k)
            part = dot(lhs[...], rhs2[sl])
            at_rows = pl.ds(pl.multiple_of(sl * ROWS + i * RB, RB), RB)
            if u == 0:
                acc2[at_rows, :] = part
            else:
                acc2[at_rows, :] += part

        loop(2, rows2)
        run2(after[n])
        if n == 4:
            for i in range(4):
                close(0, i)
            lgot[ts] = lm[0]
            c_l = [xchg(23, 1, lm.at[0], lgot.at[ts])]
    for hh in range(2):
        close(1, 2 * hh)
        close(1, 2 * hh + 1)
        for e in (0, 2):
            c_l.append(xchg(20 + 4 * hh + e, e, lm.at[1, :, h[hh]], lgot.at[ts, :, h[hh]]))

    for cp in c_l:
        cp.wait_recv()
    for k in range(4):
        out[CQ * k : CQ * k + CQ, :] = lgot[k, 0:CQ, :].astype(F32)

    for t in range(4):
        drain1(t)
    for t in range(3):
        drain2(t)
    for cp in started:
        cp.wait_send()


def per_device(
    features, self_weight1, neigh_weight1, need_first, count_first, adjacency_first,
    self_weight2, neigh_weight2, need_second, count_second, adjacency_second, seed_rows,
):
    vm = pl.BlockSpec(memory_space=pltpu.VMEM)
    sm = pl.BlockSpec(memory_space=pltpu.SMEM)
    dma = pltpu.SemaphoreType.DMA
    logits = pl.pallas_call(
        kernel,
        out_shape=jax.ShapeDtypeStruct((172, ROWS), F32),
        in_specs=[sm] * 4 + [vm] * 8 + [pl.BlockSpec(memory_space=pl.ANY)] * 2,
        out_specs=vm,
        scratch_shapes=[
            pltpu.VMEM((4, 2, 8, 16, 128), BF),
            pltpu.VMEM((ROWS, WORDS), BF),
            pltpu.VMEM((ROWS, WORDS), BF),
            pltpu.VMEM((ROWS, 128), BF),
            pltpu.VMEM((384, 128), BF),
            pltpu.VMEM((ROWS, WORDS), I32),
            pltpu.VMEM((ROWS, WORDS), I32),
            pltpu.VMEM((2048, 128), F32),
            pltpu.VMEM((128, 128), F32),
            *[pltpu.VMEM((256, 16, 128), BF)] * 4,
            *[pltpu.VMEM((256, 2, 16, 128), BF)] * 3,
            pltpu.VMEM((ROWS, WORDS), BF),
            pltpu.VMEM((ROWS, WORDS), BF),
            pltpu.VMEM((ROWS, 128), BF),
            pltpu.VMEM((4, 384, 128), BF),
            pltpu.VMEM((1, 64), I32),
            pltpu.VMEM((1, 64), I32),
            pltpu.SMEM((1, 64), I32),
            pltpu.SMEM((1, 64), I32),
            pltpu.VMEM((4, 8, 16, 128), BF),
            pltpu.VMEM((4, 128, 128), BF),
            pltpu.VMEM((4, 128, 128), BF),
            pltpu.VMEM((2 * ROWS, 128), F32),
            pltpu.VMEM((2 * ROWS, 128), F32),
            pltpu.VMEM((2 * ROWS, 256), F32),
            pltpu.VMEM((2 * ROWS, 128), F32),
            pltpu.VMEM((RB, 5 * WORDS), BF),
            pltpu.VMEM((2, 4 * WORDS, 128), BF),
            pltpu.VMEM((2, 5 * WORDS, 256), BF),
            pltpu.VMEM((2048, 128), BF),
            pltpu.VMEM((2, 512, 256), BF),
            pltpu.VMEM((4, 128, 256), BF),
            pltpu.VMEM((4, 4, 128, 128), BF),
            pltpu.VMEM((4, 4, 128, 128), BF),
            pltpu.VMEM((2, 48, ROWS), BF),
            pltpu.VMEM((4, 48, ROWS), BF),
            dma((4, 16)), dma((4,)), dma((4,)),
            dma((3, 16)), dma((3,)), dma((3,)),
            dma((27,)), dma((27,)), dma((4,)),
        ],
        compiler_params=pltpu.CompilerParams(
            collective_id=0, has_side_effects=True, vmem_limit_bytes=60 * 2**20
        ),
    )(
        need_first, need_second, count_first, count_second, need_first, need_second,
        features.T, self_weight1, neigh_weight1, self_weight2.T, neigh_weight2.T,
        seed_rows.reshape(8, 128), adjacency_first, adjacency_second,
    )
    return logits.T


def solution(mesh):
    both = P(("dom", "batch"))
    rows = P(("dom", "batch"), None)
    wide = P("col", "batch")
    placed = (
        P("dom", "col"), wide, wide, rows, both, rows, wide, wide, rows, both, rows, both,
    )
    return jax.shard_map(
        per_device, mesh=mesh, in_specs=placed, out_specs=rows, check_vma=False
    )
```
